128 devices in a mesh: rep: 16 (over x_lo, y, core), tp: 8 (over z, x_hi).
Axes of the slice: x: 4 (x_hi: 2, x_lo: 2; x = x_hi * 2 + x_lo), y: 4, z: 4, core: 2. Of those that a mesh axis runs over, the one named last changes fastest.
Arguments:
- tokens: bfloat16 [16384, 1280], P(('rep', 'tp')), may hold values from -6 to 6
- view_ids: int32 [64, 4], P('rep'), may hold values from 0 to 31
- time_ids: int32 [64], P('rep'), may hold values from 0 to 999
- camera_table: float32 [32, 1280], replicated, may hold values from -6 to 6
- norm_attn: float32 [2, 1280], replicated, may hold values from 0.1 to 1.9
- norm_ffn: float32 [2, 1280], replicated, may hold values from 0.1 to 1.9
- w_query: bfloat16 [2, 1280, 1280], P(None, ('rep', 'tp')), may hold values from -0.1677051 to 0.1677051
- w_key: bfloat16 [2, 1280, 1280], P(None, ('rep', 'tp')), may hold values from -6.764106 to 6.764106
- w_value: bfloat16 [2, 1280, 1280], P(None, ('rep', 'tp')), may hold values from -0.15625 to 0.15625
- w_out: bfloat16 [2, 1280, 1280], P(None, ('rep', 'tp')), may hold values from -0.15625 to 0.15625
- w_gate: bfloat16 [2, 1280, 5120], P(None, ('rep', 'tp')), may hold values from -0.15625 to 0.15625
- w_up: bfloat16 [2, 1280, 5120], P(None, ('rep', 'tp')), may hold values from -0.15625 to 0.15625
- w_down: bfloat16 [2, 1280, 5120], P(None, ('rep', 'tp')), may hold values from -0.078125 to 0.078125
Outputs:
- denoised: bfloat16 [16384, 1280], P(('rep', 'tp'))
The draws below stay inside these ranges and needn't reach their ends.
All inputs are finite; a program needn't handle non-finite values.
Results may differ from the reference program's by a relative error of at most 0.035.
Values may be sent and summed in bfloat16 or wider, within the bound.
A program may use at most 128 MiB of HBM per device.

```python
import math
import jax
import jax.numpy as jnp
from jax import lax

D = 1280
FF = 5120
HEADS = 8
VIEWS = 4
HW = 64
LAYERS = 2
NPOSE = 32
CAMS = 64
ROWS = 16384
N_TP = 8


def query_base(key):
    base = jax.random.normal(jax.random.fold_in(key, 11), (LAYERS, D, D), jnp.float32)
    return jnp.clip(base, -6.0, 6.0) * D ** (-0.5)


def draw_w_query(key, part):
    return query_base(key).astype(jnp.bfloat16)


def draw_w_key(key, part):
    other = jax.random.normal(jax.random.fold_in(key, 12), (LAYERS, D, D), jnp.float32)
    other = jnp.clip(other, -6.0, 6.0) * D ** (-0.5)
    return other.astype(jnp.bfloat16)


def touch_ends(drawn, own_key, low, high):
    dims = drawn.shape
    spot = [jax.random.randint(jax.random.fold_in(own_key, axis), (), 0, dims[axis]) for axis in range(len(dims))]
    drawn = drawn.at[tuple(spot)].set(low)
    longest = dims.index(max(dims))
    spot[longest] = (spot[longest] + 1) % dims[longest]
    return drawn.at[tuple(spot)].set(high)


def block_scale(rng, dims, shards, smallest, top_value):
    loudness = 1.0
    for dim, parts in shards:
        draws = jax.random.uniform(jax.random.fold_in(jax.random.fold_in(rng, 6), dim), (parts,), jnp.float32, smallest / len(shards), top_value / len(shards))
        loudness = loudness * jnp.repeat(jnp.exp(draws), dims[dim] // parts).reshape((-1,) + (1,) * (len(dims) - 1 - dim))
    return loudness


def gaussian(key, shape, scale, limit, shards=(), kind=jnp.bfloat16):
    values = jax.random.normal(key, shape, jnp.float32) * scale
    if len(shards) > 0:
        values = block_scale(key, shape, shards, -0.22, 0.18) * values
    return jnp.clip(values, min=-limit, max=limit).astype(kind)


def setup_inputs(seed: int = 0) -> dict:
    streams_of = jax.random.split(jax.random.key(seed), 14)
    tokens = gaussian(streams_of[0], (ROWS, D), 1.0, 6.0, ((0, 128),))
    view_ids = touch_ends(jax.random.randint(streams_of[1], (CAMS, VIEWS), 0, NPOSE), jax.random.fold_in(streams_of[1], 1), 0, NPOSE - 1).astype(jnp.int32)
    time_ids = touch_ends(jax.random.randint(streams_of[2], (CAMS,), 0, 1000), jax.random.fold_in(streams_of[2], 1), 0, 999).astype(jnp.int32)
    camera_table = gaussian(streams_of[3], (NPOSE, D), 1.0, 6.0, (), jnp.float32)
    norm_attn = jnp.clip(1.0 + 0.18 * jax.random.normal(streams_of[4], (LAYERS, D), jnp.float32), 0.1, 1.9)
    norm_ffn = jnp.clip(1.0 + 0.18 * jax.random.normal(streams_of[5], (LAYERS, D), jnp.float32), 0.1, 1.9)
    w_query = draw_w_query(jax.random.fold_in(streams_of[13], 71), 0)
    w_key = draw_w_key(jax.random.fold_in(streams_of[13], 71), 0)
    w_value = gaussian(streams_of[8], (LAYERS, D, D), D ** -0.5, 0.15625, ((1, 128),))
    w_out = gaussian(streams_of[9], (LAYERS, D, D), D ** -0.5, 0.15625, ((1, 128),))
    w_gate = gaussian(streams_of[10], (LAYERS, D, FF), D ** -0.5, 0.15625, ((1, 128),))
    w_up = gaussian(streams_of[11], (LAYERS, D, FF), D ** -0.5, 0.15625, ((1, 128),))
    w_down = gaussian(streams_of[12], (LAYERS, D, FF), FF ** -0.5, 0.078125, ((1, 128),))
    return dict(tokens=tokens, view_ids=view_ids, time_ids=time_ids, camera_table=camera_table, norm_attn=norm_attn, norm_ffn=norm_ffn, w_query=w_query, w_key=w_key, w_value=w_value, w_out=w_out, w_gate=w_gate, w_up=w_up, w_down=w_down)


def layer_norm(activations, gain_vector):
    average = lax.optimization_barrier(jnp.mean(activations, axis=-1, keepdims=True))
    centred = activations - average
    spread = lax.optimization_barrier(jnp.mean(centred * centred, axis=-1, keepdims=True))
    return (centred * lax.rsqrt(spread + 1e-05) * gain_vector).astype(jnp.bfloat16)

def time_code(step_ids, width):
    half_width = width // 2
    frequency = jnp.exp(-math.log(10000.0) * jnp.arange(half_width, dtype=jnp.float32) / half_width)
    angles = step_ids.astype(jnp.float32)[:, None] * frequency[None, :]
    return jnp.concatenate([jnp.cos(angles), jnp.sin(angles)], axis=1)

def split_sum(mixed_rows, weight):
    row_count = mixed_rows.shape[0]
    inner_width = mixed_rows.shape[1] // N_TP
    left_side = mixed_rows.astype(jnp.float32).reshape(row_count, N_TP, inner_width)
    right_side = weight.astype(jnp.float32).reshape(weight.shape[0], N_TP, inner_width)
    term_rows = jnp.einsum('snc,onc->nso', left_side, right_side).astype(jnp.bfloat16)
    term_rows = lax.optimization_barrier(term_rows)
    return lax.optimization_barrier(jnp.sum(term_rows.astype(jnp.float32), axis=0))

def attention(query_rows, key_rows, value_rows):
    seq_len = query_rows.shape[0]
    head_size = D // HEADS
    query_heads = query_rows.astype(jnp.float32).reshape(seq_len, HEADS, head_size)
    key_heads = key_rows.astype(jnp.float32).reshape(seq_len, HEADS, head_size)
    value_heads = value_rows.astype(jnp.float32).reshape(seq_len, HEADS, head_size)
    scores = jnp.einsum('qhd,khd->hqk', query_heads, key_heads) * head_size ** (-0.5)
    peak = lax.optimization_barrier(jnp.max(scores, axis=-1, keepdims=True))
    expons = jnp.exp(scores - peak)
    attn_probs = (expons / lax.optimization_barrier(jnp.sum(expons, axis=-1, keepdims=True))).astype(jnp.bfloat16)
    mixed_rows = jnp.einsum('hqk,khd->qhd', attn_probs.astype(jnp.float32), value_heads)
    return mixed_rows.astype(jnp.bfloat16).reshape(seq_len, D)

def reference(tokens, view_ids, time_ids, camera_table, norm_attn, norm_ffn, w_query, w_key, w_value, w_out, w_gate, w_up, w_down):
    seq_len = VIEWS * HW
    set_count = tokens.shape[0] // seq_len
    blocks = tokens.reshape(set_count, seq_len, D)

    def one_set(packed):
        block, views_here, step_here = packed
        camera = jnp.repeat(camera_table[views_here], HW, axis=0)
        stream = block.astype(jnp.float32) + camera + time_code(step_here[None], D)
        for layer_index in range(LAYERS):
            normed = layer_norm(stream, norm_attn[layer_index])
            query_rows = jnp.dot(normed, w_query[layer_index], preferred_element_type=jnp.float32).astype(jnp.bfloat16)
            key_rows = jnp.dot(normed, w_key[layer_index], preferred_element_type=jnp.float32).astype(jnp.bfloat16)
            value_rows = jnp.dot(normed, w_value[layer_index], preferred_element_type=jnp.float32).astype(jnp.bfloat16)
            mixed_rows = attention(query_rows, key_rows, value_rows)
            stream = stream + split_sum(mixed_rows, w_out[layer_index])
            normed = layer_norm(stream, norm_ffn[layer_index])
            gate_part = jnp.dot(normed, w_gate[layer_index], preferred_element_type=jnp.float32)
            up_part = jnp.dot(normed, w_up[layer_index], preferred_element_type=jnp.float32)
            hidden = (jax.nn.gelu(gate_part, approximate=False) * up_part).astype(jnp.bfloat16)
            stream = stream + split_sum(hidden, w_down[layer_index])
        return stream.astype(jnp.bfloat16)
    result = lax.map(one_set, (blocks, view_ids, time_ids))
    return result.reshape(tokens.shape[0], D)
```

```python
import functools
import math

import jax
import jax.numpy as jnp
import numpy as np
from jax import lax
from jax.experimental import pallas as pl
from jax.experimental.pallas import tpu as pltpu
from jax.sharding import PartitionSpec as P

D = 1280
HEADS = 8
HEAD = 160
VIEWS = 4
HW = 64
LAYERS = 2
ROWS = 128
UNITS = 8
UNIT = 640
MESH = pl.DeviceIdType.MESH
F32 = jnp.float32
BF16 = jnp.bfloat16


def channel_order():
    k = np.arange(D)
    block, rest = k // 80, k % 80
    z, y = block // 4, block % 4
    source, row = rest // 10, rest % 10
    x, core = source // 2, source % 2
    device = (x % 2) * 64 + y * 16 + core * 8 + z * 2 + x // 2
    return (device * 10 + row).astype(np.int32)


def row_packer():
    take = np.zeros((80, 128), np.float32)
    for i in range(80):
        take[i, i // 10 * 16 + i % 10] = 1.0
    return take


def nt_dot(a, b):
    return lax.dot_general(a, b, (((1,), (1,)), ((), ())), preferred_element_type=F32)


def kernel(
    tok_ref,
    aux_ref,
    order_ref,
    take_ref,
    wp_ref,
    out_ref,
    w,
    w2,
    a2a,
    perm,
    aux,
    stream,
    xg,
    mixed,
    hid,
    pst,
    rs,
    wsend,
    wrecv,
    asend,
    arecv,
    gsend,
    grecv,
    rsend,
    rrecv,
):
    r, t = lax.axis_index("rep"), lax.axis_index("tp")
    x = (t % 2) * 2 + r // 8
    y = (r // 2) % 4
    c = r % 2
    z = t // 2
    me8 = x * 2 + c

    def dev(x_, y_, z_, c_):
        return ((x_ % 2) * 8 + y_ * 2 + c_, z_ * 2 + x_ // 2)

    ahead = 1 - 2 * c

    def front(i):
        return (i + ahead + 4) % 4

    def back(i):
        return (i - ahead + 4) % 4

    def opposite(i):
        return (i + 2) % 4

    def slot(x_):
        return (x_ % 2) * 2 + x_ // 2

    x_front, x_back = dev(front(x), y, z, c), dev(back(x), y, z, c)
    y_front, y_back = dev(x, front(y), z, c), dev(x, back(y), z, c)
    z_front, z_back = dev(x, y, front(z), c), dev(x, y, back(z), c)
    partner = dev(x, y, z, 1 - c)

    def other8(offset):
        e = (me8 + offset) % 8
        return e, dev(e // 2, y, z, e % 2)

    barrier = pltpu.get_barrier_semaphore()
    for offset in range(1, 8):
        pl.semaphore_signal(barrier, inc=1, device_id=other8(offset)[1], device_id_type=MESH)
    for d in (y_front, y_back, z_front, z_back):
        pl.semaphore_signal(barrier, inc=1, device_id=d, device_id_type=MESH)
    pl.semaphore_wait(barrier, 11)

    def copy(src, dst, ss, rsem, d):
        return pltpu.make_async_remote_copy(
            src_ref=src, dst_ref=dst, send_sem=ss, recv_sem=rsem, device_id=d, device_id_type=MESH
        )

    def exchange(offset, part):
        e, d = other8(offset)
        if part == 0:
            src, dst = wp_ref.at[e, pl.ds(0, 1)], a2a.at[me8, pl.ds(0, 1)]
        else:
            src, dst = wp_ref.at[e, pl.ds(1, 7)], a2a.at[me8, pl.ds(1, 7)]
        return copy(src, dst, asend.at[offset - 1, part], arecv.at[offset - 1, part], d)

    for part in range(2):
        for offset in range(1, 8):
            exchange(offset, part).start()

    a2a[me8] = wp_ref[me8]

    def unit_rings(u):
        if u % 2 == 0:
            return (y, y_front, y_back), (z, z_front, z_back)
        return (z, z_front, z_back), (y, y_front, y_back)

    def piece(u, i1, i2):
        return w.at[u, i2, i1] if u % 2 == 0 else w.at[u, i1, i2]

    def line(u, i2):
        return w.at[u, i2] if u % 2 == 0 else w.at[u, :, i2]

    def wcopy(u, kind):
        (a, a_front, a_back), (b, b_front, b_back) = unit_rings(u)
        sems = (wsend.at[u, kind], wrecv.at[u, kind])
        if kind == 0:
            return copy(piece(u, a, b), piece(u, a, b), *sems, a_front)
        if kind == 1:
            return copy(piece(u, a, b), piece(u, a, b), *sems, a_back)
        if kind == 2:
            return copy(piece(u, back(a), b), piece(u, back(a), b), *sems, a_front)
        if kind == 3:
            return copy(line(u, b), line(u, b), *sems, b_front)
        if kind == 4:
            return copy(line(u, b), line(u, b), *sems, b_back)
        if kind == 5:
            return copy(line(u, back(b)), line(u, back(b)), *sems, b_front)
        return copy(w.at[u], w2.at[u], *sems, partner)

    def step(u, n):
        if n == 0:
            part = 0 if u == 0 else 1
            if u <= 1:
                for offset in range(1, 8):
                    exchange(offset, part).wait_recv()
            rows = a2a[:, u].reshape(128, UNIT)
            packed = jnp.dot(take_ref[...], rows, preferred_element_type=F32).astype(BF16)
            w[u, z, y] = packed
            wcopy(u, 0).start()
            wcopy(u, 1).start()
        elif n == 1:
            wcopy(u, 0).wait_recv()
            wcopy(u, 2).start()
        elif n == 2:
            wcopy(u, 1).wait_recv()
            wcopy(u, 2).wait_recv()
            wcopy(u, 3).start()
            wcopy(u, 4).start()
        elif n == 3:
            wcopy(u, 3).wait_recv()
            wcopy(u, 5).start()
        elif n == 4:
            wcopy(u, 4).wait_recv()
            wcopy(u, 5).wait_recv()
            wcopy(u, 6).start()

    todo = []
    for tick in range(UNITS + 5):
        for n in range(4, -1, -1):
            u = tick - n
            if 0 <= u < UNITS:
                todo.append((u, n))
    ready = set()

    def pump(count):
        for _ in range(min(count, len(todo))):
            step(*todo.pop(0))

    def need(u):
        while (u, 4) in todo:
            pump(1)
        if u not in ready:
            wcopy(u, 6).wait_recv()
            ready.add(u)

    pump(3)

    perm[...] = (
        lax.broadcasted_iota(jnp.int32, (D, D), 0) == order_ref[...]
    ).astype(F32).astype(BF16)
    rows = aux_ref[...]
    high = rows.astype(BF16)
    left = rows - high.astype(F32)
    middle = left.astype(BF16)
    low = (left - middle.astype(F32)).astype(BF16)
    aux[...] = (
        jnp.dot(high, perm[...], preferred_element_type=F32)
        + jnp.dot(middle, perm[...], preferred_element_type=F32)
        + jnp.dot(low, perm[...], preferred_element_type=F32)
    )
    tokens = jnp.dot(tok_ref[...], perm[...], preferred_element_type=F32)
    stream[0:HW, :] = tokens[0:HW, :] + aux[0:1, :]
    stream[HW : 2 * HW, :] = tokens[HW : 2 * HW, :] + aux[1:2, :]

    def gather_start(gain):
        rows = stream[...]
        mean = jnp.mean(rows, axis=-1, keepdims=True)
        centred = rows - mean
        spread = jnp.mean(centred * centred, axis=-1, keepdims=True)
        xg[slot(x)] = (centred * lax.rsqrt(spread + 1e-05) * gain).astype(BF16)
        gcopy(0).start()
        gcopy(1).start()

    def gcopy(kind):
        sems = (gsend.at[kind], grecv.at[kind])
        if kind == 0:
            return copy(xg.at[slot(x)], xg.at[slot(x)], *sems, x_front)
        if kind == 1:
            return copy(xg.at[slot(x)], xg.at[slot(x)], *sems, x_back)
        return copy(xg.at[slot(back(x))], xg.at[slot(back(x))], *sems, x_front)

    def gather_finish():
        gcopy(0).wait_recv()
        gcopy(2).start()
        pump(2)
        gcopy(1).wait_recv()
        gcopy(2).wait_recv()
        for kind in range(3):
            gcopy(kind).wait_send()

    def rcopy(kind):
        target = x_back if kind == 1 else x_front
        return copy(pst.at[kind], rs.at[kind], rsend.at[kind], rrecv.at[kind], target)

    def reduce(partial):
        pst[0] = partial(slot(opposite(x))).astype(BF16)
        rcopy(0).start()
        pst[1] = partial(slot(back(x))).astype(BF16)
        rcopy(1).start()
        mine = partial(slot(front(x)))
        pump(2)
        rcopy(0).wait_recv()
        pst[2] = (mine + rs[0].astype(F32)).astype(BF16)
        rcopy(2).start()
        mine = partial(slot(x))
        stream[...] += mine
        pump(2)
        rcopy(1).wait_recv()
        rcopy(2).wait_recv()
        stream[...] += rs[1].astype(F32) + rs[2].astype(F32)
        for kind in range(3):
            rcopy(kind).wait_send()

    lane = lax.broadcasted_iota(jnp.int32, (256, 256), 1)

    for layer in range(LAYERS):
        attn_u, gate_u, up_u, down_u = (4 * layer + i for i in range(4))
        gather_start(aux[2 + layer : 3 + layer, :])
        need(attn_u)
        gather_finish()
        for half, held in enumerate((w, w2)):
            for pair in range(2):
                rows = xg[2 * pair : 2 * pair + 2].reshape(256, D)
                packed = jnp.dot(
                    rows, held[attn_u, :, :, :, 0:512].reshape(D, 512), preferred_element_type=F32
                )
                query = jnp.where(lane < HEAD, packed[:, 0:256], 0.0).astype(BF16)
                key = pltpu.roll(packed[:, 128:384], 224, 1).astype(BF16)
                value = jnp.where(lane >= 96, pltpu.roll(packed[:, 256:512], 32, 1), 0.0).astype(BF16)
                scores = nt_dot(query, key) * HEAD ** (-0.5)
                peak = jnp.max(scores, axis=-1, keepdims=True)
                expons = jnp.exp(scores - peak)
                probs = (expons / jnp.sum(expons, axis=-1, keepdims=True)).astype(BF16)
                heads = jnp.dot(probs, value, preferred_element_type=F32).astype(BF16)
                mixed[half, 2 * pair : 2 * pair + 2] = heads.reshape(2, ROWS, 256)

        def attn_partial(s):
            total = nt_dot(mixed[0, s], w[attn_u, :, :, :, 384:640].reshape(D, 256))
            return total + nt_dot(mixed[1, s], w2[attn_u, :, :, :, 384:640].reshape(D, 256))

        reduce(attn_partial)
        gather_start(aux[4 + layer : 5 + layer, :])
        need(gate_u)
        need(up_u)
        gather_finish()
        rows = xg[...].reshape(4 * ROWS, D)
        for half, held in enumerate((w, w2)):
            for j in range(5):
                cols = slice(128 * j, 128 * j + 128)
                both = jnp.concatenate(
                    [
                        held[gate_u, :, :, :, cols].reshape(D, 128),
                        held[up_u, :, :, :, cols].reshape(D, 128),
                    ],
                    axis=1,
                )
                packed = jnp.dot(rows, both, preferred_element_type=F32)
                gate = packed[:, 0:128]
                act = 0.5 * gate * (1.0 + lax.erf(gate * math.sqrt(0.5)))
                hid[half, :, :, cols] = (act * packed[:, 128:256]).astype(BF16).reshape(4, ROWS, 128)
        need(down_u)

        def ffn_partial(s):
            total = nt_dot(hid[0, s], w[down_u].reshape(D, UNIT))
            return total + nt_dot(hid[1, s], w2[down_u].reshape(D, UNIT))

        reduce(ffn_partial)

    out_ref[...] = nt_dot(stream[...].astype(BF16), perm[...]).astype(BF16)

    for part in range(2):
        for offset in range(1, 8):
            exchange(offset, part).wait_send()
    for u in range(UNITS):
        for kind in range(7):
            wcopy(u, kind).wait_send()


def conditioning(view_ids, time_ids, camera_table):
    t = lax.axis_index("tp")
    views = lax.dynamic_slice(view_ids, (t // 2, t % 2 * 2), (1, 2)).reshape(2)
    step = lax.dynamic_slice(time_ids, (t // 2,), (1,))
    half = D // 2
    frequency = jnp.exp(-math.log(10000.0) * jnp.arange(half, dtype=F32) / half)
    angles = step.astype(F32)[:, None] * frequency[None, :]
    code = jnp.concatenate([jnp.cos(angles), jnp.sin(angles)], axis=1)
    return camera_table[views] + code


def send_layout(weights):
    small = [a.reshape(2, 10, 8, HEAD) for a in weights[:4]]
    attn = jnp.concatenate(small, axis=3)[:, None]
    big = [a.reshape(2, 10, 8, UNIT)[:, None] for a in weights[4:]]
    units = jnp.concatenate([attn, *big], axis=1)
    units = units.transpose(3, 0, 1, 2, 4).reshape(8, UNITS, 10, UNIT)
    return jnp.pad(units, ((0, 0), (0, 0), (0, 6), (0, 0)))


def body(tokens, view_ids, time_ids, camera_table, norm_attn, norm_ffn, *weights):
    cond = conditioning(view_ids, time_ids, camera_table)
    aux = jnp.concatenate([cond, norm_attn, norm_ffn, jnp.zeros((2, D), F32)], axis=0)
    order = jnp.asarray(channel_order())[None, :]
    take = jnp.asarray(row_packer(), BF16)
    vmem = pl.BlockSpec(memory_space=pltpu.VMEM)
    dma = pltpu.SemaphoreType.DMA
    return pl.pallas_call(
        kernel,
        out_shape=jax.ShapeDtypeStruct((ROWS, D), BF16),
        in_specs=[vmem] * 5,
        out_specs=vmem,
        scratch_shapes=[
            pltpu.VMEM((UNITS, 4, 4, 80, UNIT), BF16),
            pltpu.VMEM((UNITS, 4, 4, 80, UNIT), BF16),
            pltpu.VMEM((8, UNITS, 16, UNIT), BF16),
            pltpu.VMEM((D, D), BF16),
            pltpu.VMEM((8, D), F32),
            pltpu.VMEM((ROWS, D), F32),
            pltpu.VMEM((4, ROWS, D), BF16),
            pltpu.VMEM((2, 4, ROWS, 256), BF16),
            pltpu.VMEM((2, 4, ROWS, UNIT), BF16),
            pltpu.VMEM((3, ROWS, D), BF16),
            pltpu.VMEM((3, ROWS, D), BF16),
            dma((UNITS, 7)),
            dma((UNITS, 7)),
            dma((7, 2)),
            dma((7, 2)),
            dma((3,)),
            dma((3,)),
            dma((3,)),
            dma((3,)),
        ],
        compiler_params=pltpu.CompilerParams(
            collective_id=0, has_side_effects=True, vmem_limit_bytes=60 * 1024 * 1024
        ),
    )(tokens, aux, order, take, send_layout(weights))


def solution(mesh):
    return jax.shard_map(
        body,
        mesh=mesh,
        in_specs=(
            P(("rep", "tp"), None),
            P("rep", None),
            P("rep"),
            P(),
            P(),
            P(),
            *([P(None, ("rep", "tp"), None)] * 7),
        ),
        out_specs=P(("rep", "tp"), None),
        check_vma=False,
    )
```

```python
import functools
import math

import jax
import jax.numpy as jnp
import numpy as np
from jax import lax
from jax.experimental import pallas as pl
from jax.experimental.pallas import tpu as pltpu
from jax.sharding import PartitionSpec as P

D = 1280
HEADS = 8
HEAD = 160
VIEWS = 4
HW = 64
LAYERS = 2
ROWS = 128
UNITS = 8
UNIT = 640
MESH = pl.DeviceIdType.MESH
F32 = jnp.float32
BF16 = jnp.bfloat16


def channel_order():
    k = np.arange(D)
    block, rest = k // 80, k % 80
    z, y = block // 4, block % 4
    source, row = rest // 10, rest % 10
    x, core = source // 2, source % 2
    device = (x % 2) * 64 + y * 16 + core * 8 + z * 2 + x // 2
    return (device * 10 + row).astype(np.int32)


def row_sorter():
    take = np.zeros((160, 160), np.float32)
    for layer in range(2):
        for i in range(80):
            take[layer * 80 + i, i * 2 + layer] = 1.0
    return take


def nt_dot(a, b):
    return lax.dot_general(a, b, (((1,), (1,)), ((), ())), preferred_element_type=F32)


def kernel(
    tok_ref,
    view_ref,
    time_ref,
    table_ref,
    norm_attn_ref,
    norm_ffn_ref,
    order_ref,
    sort_ref,
    wq_ref,
    wk_ref,
    wv_ref,
    wo_ref,
    wg_ref,
    wu_ref,
    wd_ref,
    out_ref,
    w,
    w2,
    a2a,
    parts,
    perm,
    raw,
    aux,
    stream,
    xg,
    queries,
    keys,
    values,
    mixed,
    hid,
    terms,
    pst,
    rs,
    wsend,
    wrecv,
    asend,
    arecv,
    lsem,
    gsend,
    grecv,
    rsend,
    rrecv,
):
    r, t = lax.axis_index("rep"), lax.axis_index("tp")
    x = (t % 2) * 2 + r // 8
    y = (r // 2) % 4
    c = r % 2
    z = t // 2
    me8 = x * 2 + c

    def dev(x_, y_, z_, c_):
        return ((x_ % 2) * 8 + y_ * 2 + c_, z_ * 2 + x_ // 2)

    ahead = 1 - 2 * c

    def front(i):
        return (i + ahead + 4) % 4

    def back(i):
        return (i - ahead + 4) % 4

    def opposite(i):
        return (i + 2) % 4

    def slot(x_):
        return (x_ % 2) * 2 + x_ // 2

    x_front, x_back = dev(front(x), y, z, c), dev(back(x), y, z, c)
    y_front, y_back = dev(x, front(y), z, c), dev(x, back(y), z, c)
    z_front, z_back = dev(x, y, front(z), c), dev(x, y, back(z), c)
    partner = dev(x, y, z, 1 - c)

    def other8(offset):
        e = (me8 + offset) % 8
        return e, dev(e // 2, y, z, e % 2)

    barrier = pltpu.get_barrier_semaphore()
    for offset in range(1, 8):
        pl.semaphore_signal(barrier, inc=1, device_id=other8(offset)[1], device_id_type=MESH)
    for d in (y_front, y_back, z_front, z_back):
        pl.semaphore_signal(barrier, inc=1, device_id=d, device_id_type=MESH)

    rows = [ref[...].astype(F32) for ref in (wq_ref, wk_ref, wv_ref, wo_ref)]
    for e in range(8):
        cut = [a[:, :, HEAD * e : HEAD * e + HEAD] for a in rows]
        parts[e] = jnp.concatenate(cut, axis=2).astype(BF16)

    perm[...] = (
        lax.broadcasted_iota(jnp.int32, (D, D), 0) == order_ref[...]
    ).astype(F32).astype(BF16)
    frequency = jnp.exp(
        lax.broadcasted_iota(jnp.int32, (1, D // 2), 1).astype(F32) * (-math.log(10000.0) / (D // 2))
    )
    angles = time_ref[t // 2].astype(F32) * frequency
    code = jnp.concatenate([jnp.cos(angles), jnp.sin(angles)], axis=1)
    for v in range(2):
        pose = view_ref[t // 2, (t % 2) * 2 + v]
        raw[v : v + 1, :] = table_ref[pl.ds(pose, 1), :] + code
    raw[2:4, :] = norm_attn_ref[...]
    raw[4:6, :] = norm_ffn_ref[...]
    raw[6:8, :] = jnp.zeros((2, D), F32)
    rows = raw[...]
    high = rows.astype(BF16)
    left = rows - high.astype(F32)
    middle = left.astype(BF16)
    low = (left - middle.astype(F32)).astype(BF16)
    aux[...] = (
        jnp.dot(high, perm[...], preferred_element_type=F32)
        + jnp.dot(middle, perm[...], preferred_element_type=F32)
        + jnp.dot(low, perm[...], preferred_element_type=F32)
    )
    tokens = jnp.dot(tok_ref[...], perm[...], preferred_element_type=F32)
    for h in range(2):
        stream[h] = tokens[HW * h : HW * h + HW, :] + aux[h : h + 1, :]

    pl.semaphore_wait(barrier, 11)

    def copy(src, dst, ss, rsem, d):
        return pltpu.make_async_remote_copy(
            src_ref=src, dst_ref=dst, send_sem=ss, recv_sem=rsem, device_id=d, device_id_type=MESH
        )

    def shard(e, part):
        if part == 0:
            return parts.at[e]
        ref = (wg_ref, wu_ref, wd_ref)[part - 1]
        return ref.at[:, :, pl.ds(pl.multiple_of(e * UNIT, UNIT), UNIT)]

    def exchange(offset, part):
        e, d = other8(offset)
        sems = (asend.at[offset - 1, part], arecv.at[offset - 1, part])
        return copy(shard(e, part), a2a.at[part, me8], *sems, d)

    def keep(part):
        return pltpu.make_async_copy(shard(me8, part), a2a.at[part, me8], lsem.at[part])

    for part in range(4):
        for offset in range(1, 8):
            exchange(offset, part).start()
        keep(part).start()

    def rings(h):
        if h == 0:
            return (y, y_front, y_back), (z, z_front, z_back)
        return (z, z_front, z_back), (y, y_front, y_back)

    def lanes(u, h):
        cut = 384 if u % 2 == 0 else 256
        return pl.ds(0, cut) if h == 0 else pl.ds(cut, UNIT - cut)

    def piece(ref, u, h, i1, i2):
        return ref.at[u, i2, i1, :, lanes(u, h)] if h == 0 else ref.at[u, i1, i2, :, lanes(u, h)]

    def line(ref, u, h, i2):
        return ref.at[u, i2, :, :, lanes(u, h)] if h == 0 else ref.at[u, :, i2, :, lanes(u, h)]

    def wcopy(u, h, kind):
        (a, a_front, a_back), (b, b_front, b_back) = rings(h)
        sems = (wsend.at[u, h, kind], wrecv.at[u, h, kind])
        if kind < 3:
            held = piece(w, u, h, back(a) if kind == 2 else a, b)
            return copy(held, held, *sems, a_back if kind == 1 else a_front)
        if kind < 6:
            held = line(w, u, h, back(b) if kind == 5 else b)
            return copy(held, held, *sems, b_back if kind == 4 else b_front)
        at = (b, back(b), front(b), opposite(b))[kind - 6]
        return copy(line(w, u, h, at), line(w2, u, h, at), *sems, partner)

    def step(u, n):
        if n == 0:
            if u < 4:
                keep(u).wait()
                for offset in range(1, 8):
                    exchange(offset, u).wait_recv()
                sorted_rows = jnp.dot(sort_ref[...], a2a[u].reshape(160, UNIT), preferred_element_type=F32)
                w[u, z, y] = sorted_rows[0:80].astype(BF16)
                w[u + 4, z, y] = sorted_rows[80:160].astype(BF16)
        for h in range(2):
            if n == 0:
                wcopy(u, h, 0).start()
                wcopy(u, h, 1).start()
            elif n == 1:
                wcopy(u, h, 0).wait_recv()
                wcopy(u, h, 2).start()
            elif n == 2:
                wcopy(u, h, 1).wait_recv()
                wcopy(u, h, 2).wait_recv()
                wcopy(u, h, 3).start()
                wcopy(u, h, 4).start()
                wcopy(u, h, 6).start()
            elif n == 3:
                wcopy(u, h, 3).wait_recv()
                wcopy(u, h, 5).start()
                wcopy(u, h, 7).start()
            elif n == 4:
                wcopy(u, h, 4).wait_recv()
                wcopy(u, h, 8).start()
            elif n == 5:
                wcopy(u, h, 5).wait_recv()
                wcopy(u, h, 9).start()

    first = [(0, 0), (0, 1), (1, 0), (0, 2), (1, 1), (2, 0), (0, 3), (1, 2), (2, 1), (3, 0), (0, 4), (0, 5)]

    def due(u, n):
        while n < 3:
            u, n = u - 1, n + 1
        return 6.5 + 9.3 * (u - 1) + (0.0, 5.0, 5.5)[n - 3]

    later = [(u, n) for u in range(UNITS) for n in range(6) if (u, n) not in first]
    later.sort(key=lambda item: (due(*item), -item[1]))
    todo = [(-1.0, u, n) for u, n in first] + [(due(u, n), u, n) for u, n in later]
    ready = set()

    def advance():
        _, u, n = todo.pop(0)
        with jax.named_scope(f"pump_{u}_{n}"):
            step(u, n)

    def pump(now):
        while todo and todo[0][0] <= now:
            advance()

    def need(u):
        while any(item[1:] == (u, 5) for item in todo):
            advance()
        if u not in ready:
            with jax.named_scope(f"need_{u}"):
                for h in range(2):
                    for kind in range(6, 10):
                        wcopy(u, h, kind).wait_recv()
            ready.add(u)

    def gather_start(h, gain):
        rows = stream[h]
        mean = jnp.mean(rows, axis=-1, keepdims=True)
        centred = rows - mean
        spread = jnp.mean(centred * centred, axis=-1, keepdims=True)
        xg[h, slot(x)] = (centred * lax.rsqrt(spread + 1e-05) * gain).astype(BF16)
        gcopy(h, 0).start()
        gcopy(h, 1).start()

    def gcopy(h, kind):
        held = xg.at[h, slot(back(x) if kind == 2 else x)]
        return copy(held, held, gsend.at[h, kind], grecv.at[h, kind], x_back if kind == 1 else x_front)

    def gather_forward(h):
        gcopy(h, 0).wait_recv()
        gcopy(h, 2).start()

    def gather_finish(h):
        gcopy(h, 1).wait_recv()
        gcopy(h, 2).wait_recv()
        for kind in range(3):
            gcopy(h, kind).wait_send()

    def rcopy(h, kind):
        target = x_back if kind == 1 else x_front
        return copy(pst.at[h, kind], rs.at[h, kind], rsend.at[h, kind], rrecv.at[h, kind], target)

    def reduce_start(h, partial):
        terms[h] = partial(h).reshape(4, HW, D)
        pst[h, 0] = terms[h, slot(opposite(x))].astype(BF16)
        rcopy(h, 0).start()
        pst[h, 1] = terms[h, slot(back(x))].astype(BF16)
        rcopy(h, 1).start()

    def reduce_forward(h):
        rcopy(h, 0).wait_recv()
        pst[h, 2] = (terms[h, slot(front(x))] + rs[h, 0].astype(F32)).astype(BF16)
        rcopy(h, 2).start()

    def reduce_finish(h):
        mine = stream[h] + terms[h, slot(x)]
        rcopy(h, 1).wait_recv()
        rcopy(h, 2).wait_recv()
        stream[h] = mine + (rs[h, 1].astype(F32) + rs[h, 2].astype(F32))
        for kind in range(3):
            rcopy(h, kind).wait_send()

    lane = lax.broadcasted_iota(jnp.int32, (256, 256), 1)

    def project(h, u):
        rows = xg[h].reshape(256, D)
        for half, held in enumerate((w, w2)):
            packed = jnp.dot(rows, held[u, :, :, :, 0:512].reshape(D, 512), preferred_element_type=F32)
            query = jnp.where(lane < HEAD, packed[:, 0:256], 0.0)
            key = pltpu.roll(packed[:, 128:384], 224, 1)
            value = jnp.where(lane >= 96, pltpu.roll(packed[:, 256:512], 32, 1), 0.0)
            queries[half, h] = query.astype(BF16).reshape(2, 128, 256)
            keys[half, :, h] = key.astype(BF16).reshape(2, 128, 256)
            values[half, :, h] = value.astype(BF16).reshape(2, 128, 256)

    def attend(h):
        for half in range(2):
            for pair in range(2):
                scores = nt_dot(queries[half, h, pair], keys[half, pair].reshape(256, 256))
                scores = scores * HEAD ** (-0.5)
                peak = jnp.max(scores, axis=-1, keepdims=True)
                expons = jnp.exp(scores - peak)
                probs = (expons / jnp.sum(expons, axis=-1, keepdims=True)).astype(BF16)
                heads = jnp.dot(probs, values[half, pair].reshape(256, 256), preferred_element_type=F32)
                mixed[half, h, pair] = heads.astype(BF16)

    def feed(h, gate_u, up_u, now):
        rows = xg[h].reshape(256, D)
        for half, held in enumerate((w, w2)):
            pump(now + 1.4 * half)
            for j in range(5):
                cols = slice(128 * j, 128 * j + 128)
                both = jnp.concatenate(
                    [
                        held[gate_u, :, :, :, cols].reshape(D, 128),
                        held[up_u, :, :, :, cols].reshape(D, 128),
                    ],
                    axis=1,
                )
                packed = jnp.dot(rows, both, preferred_element_type=F32)
                gate = packed[:, 0:128]
                act = 0.5 * gate * (1.0 + lax.erf(gate * math.sqrt(0.5)))
                hid[half, h, :, cols] = (act * packed[:, 128:256]).astype(BF16)

    for _ in range(3):
        advance()
    for h in range(2):
        gather_start(h, aux[2:3, :])
    for layer in range(LAYERS):
        attn_u, gate_u, up_u, down_u = (4 * layer + i for i in range(4))
        base = 48 * layer

        def attn_partial(h):
            total = nt_dot(
                mixed[0, h].reshape(256, 256), w[attn_u, :, :, :, 384:640].reshape(D, 256)
            )
            return total + nt_dot(
                mixed[1, h].reshape(256, 256), w2[attn_u, :, :, :, 384:640].reshape(D, 256)
            )

        def ffn_partial(h):
            total = nt_dot(hid[0, h], w[down_u].reshape(D, UNIT))
            return total + nt_dot(hid[1, h], w2[down_u].reshape(D, UNIT))

        def both_reduced(gain, now):
            for h in range(2):
                reduce_forward(h)
                pump(now + 4.5 + 2 * h)
            for h in range(2):
                reduce_finish(h)
                if gain is not None:
                    gather_start(h, gain)
                pump(now + 10 + 3.5 * h)

        need(attn_u)
        pump(base)
        for h in range(2):
            gather_forward(h)
            pump(base + 2 + 2 * h)
        for h in range(2):
            gather_finish(h)
            project(h, attn_u)
            pump(base + 5.5 + 1.5 * h)
        for h in range(2):
            attend(h)
            pump(base + 8 + 1.7 * h)
            reduce_start(h, attn_partial)
            pump(base + 8.8 + 1.7 * h)
        both_reduced(aux[4 + layer : 5 + layer, :], base + 10.5)
        for h in range(2):
            gather_forward(h)
            pump(base + 27 + 2.5 * h)
        need(gate_u)
        need(up_u)
        for h in range(2):
            gather_finish(h)
            feed(h, gate_u, up_u, base + 31.5 + 4 * h)
            if h == 0:
                need(down_u)
            pump(base + 34 + 4 * h)
            reduce_start(h, ffn_partial)
            pump(base + 35.3 + 4 * h)
        both_reduced(aux[3:4, :] if layer == 0 else None, base + 39)

    for h in range(2):
        out_ref[HW * h : HW * h + HW, :] = nt_dot(stream[h].astype(BF16), perm[...]).astype(BF16)

    for part in range(4):
        for offset in range(1, 8):
            exchange(offset, part).wait_send()
    for u in range(UNITS):
        for h in range(2):
            for kind in range(10):
                wcopy(u, h, kind).wait_send()


def body(tokens, view_ids, time_ids, camera_table, norm_attn, norm_ffn, *weights):
    order = jnp.asarray(channel_order())[None, :]
    sorter = jnp.asarray(row_sorter(), BF16)
    weights = [a.transpose(1, 0, 2) for a in weights]
    vmem = pl.BlockSpec(memory_space=pltpu.VMEM)
    smem = pl.BlockSpec(memory_space=pltpu.SMEM)
    dma = pltpu.SemaphoreType.DMA
    return pl.pallas_call(
        kernel,
        out_shape=jax.ShapeDtypeStruct((ROWS, D), BF16),
        in_specs=[vmem, smem, smem] + [vmem] * 9 + [pl.BlockSpec(memory_space=pl.ANY)] * 3,
        out_specs=vmem,
        scratch_shapes=[
            pltpu.VMEM((UNITS, 4, 4, 80, UNIT), BF16),
            pltpu.VMEM((UNITS, 4, 4, 80, UNIT), BF16),
            pltpu.VMEM((4, 8, 10, LAYERS, UNIT), BF16),
            pltpu.VMEM((8, 10, LAYERS, UNIT), BF16),
            pltpu.VMEM((D, D), BF16),
            pltpu.VMEM((8, D), F32),
            pltpu.VMEM((8, D), F32),
            pltpu.VMEM((2, HW, D), F32),
            pltpu.VMEM((2, 4, HW, D), BF16),
            pltpu.VMEM((2, 2, 2, 128, 256), BF16),
            pltpu.VMEM((2, 2, 2, 128, 256), BF16),
            pltpu.VMEM((2, 2, 2, 128, 256), BF16),
            pltpu.VMEM((2, 2, 2, 128, 256), BF16),
            pltpu.VMEM((2, 2, 256, UNIT), BF16),
            pltpu.VMEM((2, 4, HW, D), F32),
            pltpu.VMEM((2, 3, HW, D), BF16),
            pltpu.VMEM((2, 3, HW, D), BF16),
            dma((UNITS, 2, 10)),
            dma((UNITS, 2, 10)),
            dma((7, 4)),
            dma((7, 4)),
            dma((4,)),
            dma((2, 3)),
            dma((2, 3)),
            dma((2, 3)),
            dma((2, 3)),
        ],
        compiler_params=pltpu.CompilerParams(
            collective_id=0, has_side_effects=True, vmem_limit_bytes=60 * 1024 * 1024
        ),
    )(tokens, view_ids, time_ids, camera_table, norm_attn, norm_ffn, order, sorter, *weights)


def solution(mesh):
    return jax.shard_map(
        body,
        mesh=mesh,
        in_specs=(
            P(("rep", "tp"), None),
            P("rep", None),
            P("rep"),
            P(),
            P(),
            P(),
            *([P(None, ("rep", "tp"), None)] * 7),
        ),
        out_specs=P(("rep", "tp"), None),
        check_vma=False,
    )
```
